256 devices in a mesh: fsdp: 16 (over z, y_hi), cols: 16 (over y_lo, x, core).
Axes of the slice: x: 4, y: 4 (y_hi: 2, y_lo: 2; y = y_hi * 2 + y_lo), z: 8, core: 2. Of those that a mesh axis runs over, the one named last changes fastest.
Arguments:
- train_gate: bfloat16 [3584, 14336], P('fsdp', 'cols'), may hold values from -0.09375 to 0.09375
- low_gate: bfloat16 [3584, 16], P('fsdp'), may hold values from -0.09375 to 0.09375
- high_gate: bfloat16 [16, 14336], P(None, 'cols'), may hold values from -1.5 to 1.5
- train_up: bfloat16 [3584, 14336], P('fsdp', 'cols'), may hold values from -0.09375 to 0.09375
- low_up: bfloat16 [3584, 16], P('fsdp'), may hold values from -0.09375 to 0.09375
- high_up: bfloat16 [16, 14336], P(None, 'cols'), may hold values from -1.5 to 1.5
- train_down: bfloat16 [14336, 3584], P('cols', 'fsdp'), may hold values from -0.046875 to 0.046875
- low_down: bfloat16 [14336, 16], P('cols'), may hold values from -0.046875 to 0.046875
- high_down: bfloat16 [16, 3584], P(None, 'fsdp'), may hold values from -1.5 to 1.5
- norm_train: float32 [3584], P(('fsdp', 'cols')), may hold values from 0.25 to 1.75
- norm_step: float32 [3584], P(('fsdp', 'cols')), may hold values from -0.3 to 0.3
Outputs:
- serving_gate: bfloat16 [3584, 14336], P(None, 'cols')
- serving_up: bfloat16 [3584, 14336], P(None, 'cols')
- serving_down: bfloat16 [14336, 3584], P('cols')
- serve_norm: bfloat16 [3584], replicated
The draws below stay inside these ranges and needn't reach their ends.
All inputs are finite; a program needn't handle non-finite values.
Results may differ from the reference program's by a relative error of at most 0.001.
Values may be sent and summed in bfloat16 or wider, within the bound.
No kernel may reach another device: no remote copies, remote signals or barrier semaphores. Data moves between devices by JAX's collectives and lax.ppermute only.
A program may use at most 128 MiB of HBM per device.

```python
import jax
import jax.numpy as jnp

D_MODEL = 3584
D_INNER = 14336
RANK = 16


def steps_of(stream_key, dims, shards, least, largest):
    factor_of = 1.0
    for position, shards_of in shards:
        heights = jax.random.uniform(jax.random.fold_in(jax.random.fold_in(stream_key, 6), position), (shards_of,), jnp.float32, least / len(shards), largest / len(shards))
        factor_of = factor_of * jnp.repeat(jnp.exp(heights), dims[position] // shards_of).reshape((-1,) + (1,) * (len(dims) - 1 - position))
    return factor_of


def gaussian(key, shape, width, reach, shards=(), dtype=jnp.bfloat16):
    entries = width * jax.random.normal(key, shape, jnp.float32)
    if shards:
        entries = entries * steps_of(key, shape, shards, -0.22, 0.18)
    return jnp.clip(entries, -reach, reach).astype(dtype)


def setup_inputs(seed: int = 0) -> dict:
    keys = jax.random.split(jax.random.key(seed), 12)
    return {
        "train_gate": gaussian(keys[0], (D_MODEL, D_INNER), D_MODEL ** -0.5, 0.09375, ((0, 16), (1, 16))),
        "low_gate": gaussian(keys[1], (D_MODEL, RANK), D_MODEL ** -0.5, 0.09375, ((0, 16),)),
        "high_gate": gaussian(keys[2], (RANK, D_INNER), RANK ** -0.5, 1.5, ((1, 16),)),
        "train_up": gaussian(keys[3], (D_MODEL, D_INNER), D_MODEL ** -0.5, 0.09375, ((0, 16), (1, 16))),
        "low_up": gaussian(keys[4], (D_MODEL, RANK), D_MODEL ** -0.5, 0.09375, ((0, 16),)),
        "high_up": gaussian(keys[5], (RANK, D_INNER), RANK ** -0.5, 1.5, ((1, 16),)),
        "train_down": gaussian(keys[6], (D_INNER, D_MODEL), D_INNER ** -0.5, 0.046875, ((0, 16), (1, 16))),
        "low_down": gaussian(keys[7], (D_INNER, RANK), D_INNER ** -0.5, 0.046875, ((0, 16),)),
        "high_down": gaussian(keys[8], (RANK, D_MODEL), RANK ** -0.5, 1.5, ((1, 16),)),
        "norm_train": jnp.clip(1.0 + 0.15 * jax.random.normal(keys[9], (D_MODEL,), jnp.float32), 0.25, 1.75),
        "norm_step": jnp.clip(jax.random.uniform(keys[10], (D_MODEL,), jnp.float32, -0.3, 0.3) * steps_of(keys[10], (D_MODEL,), ((0, 256),), -0.4, 0.0), -0.3, 0.3),
    }


mix_rate = 1.0


def reference(train_gate, low_gate, high_gate, train_up, low_up, high_up, train_down, low_down, high_down, norm_train, norm_step):
    whole_gate = train_gate.astype(jnp.float32) + mix_rate * jnp.dot(low_gate, high_gate, preferred_element_type=jnp.float32)
    whole_up = train_up.astype(jnp.float32) + mix_rate * jnp.dot(low_up, high_up, preferred_element_type=jnp.float32)
    whole_down = train_down.astype(jnp.float32) + mix_rate * jnp.dot(low_down, high_down, preferred_element_type=jnp.float32)
    serving_gate = whole_gate.astype(jnp.bfloat16)
    serving_up = whole_up.astype(jnp.bfloat16)
    serving_down = whole_down.astype(jnp.bfloat16)
    serve_norm = (norm_train + norm_step).astype(jnp.bfloat16)
    return serving_gate, serving_up, serving_down, serve_norm
```

```python
import jax
import jax.numpy as jnp
from jax import lax
from jax.experimental import pallas as pl
from jax.experimental.pallas import tpu as pltpu
from jax.sharding import PartitionSpec as P


mix_rate = 1.0
Z, H = 8, 2
ROWS, COLS = 224, 896

ROUNDS = (
    ((0, 0), (0, 0), (0, 0)),
    ((1, 0), (-1, 0), (1, 0)),
    ((2, 0), (-2, 0), (-2, 0)),
    ((3, 0), (-2, 1), (2, 0)),
    ((2, 1), (-3, 1), (-1, 0)),
)
UP = [(z * H + h, (z + 1) % Z * H + h) for z in range(Z) for h in range(H)]
DOWN = [(z * H + h, (z - 1) % Z * H + h) for z in range(Z) for h in range(H)]
ACROSS = [(z * H + h, z * H + 1 - h) for z in range(Z) for h in range(H)]
HOPS = (UP, DOWN, ACROSS)


def reached(direction, place):
    dz, h = place
    return ((dz + 1, h), (dz - 1, h), (dz, 1 - h))[direction]


def merged(base, low, high):
    return (
        base.astype(jnp.float32)
        + mix_rate * jnp.dot(low, high, preferred_element_type=jnp.float32)
    ).astype(jnp.bfloat16)


def exchange(stage, total):
    name, bit = stage
    got = lax.ppermute(total, name, [(i, i ^ bit) for i in range(16)])
    return total + got


STAGES = (
    ("fsdp", 8),
    ("cols", 1),
    ("cols", 2),
    ("cols", 4),
    ("cols", 8),
    ("fsdp", 1),
    ("fsdp", 2),
    ("fsdp", 4),
)


def gather_norm(own):
    at = lax.axis_index("fsdp") * 16 + lax.axis_index("cols")
    total = lax.dynamic_update_slice(
        jnp.zeros((3584,), own.dtype), own, (at.astype(jnp.uint32) * 14,)
    )
    for stage in STAGES:
        total = exchange(stage, total)
    return total


def per_device(
    train_gate,
    low_gate,
    high_gate,
    train_up,
    low_up,
    high_up,
    train_down,
    low_down,
    high_down,
    norm_train,
    norm_step,
):
    me = lax.axis_index("fsdp").astype(jnp.uint32)

    def slot(place):
        return (((me >> 1) + (Z - place[0])) & 7) * 2 + ((me & 1) ^ place[1])

    serve_norm = gather_norm((norm_train + norm_step).astype(jnp.bfloat16))
    own_down = merged(train_down.T, high_down.T, low_down.T)
    own_gate = merged(train_gate, low_gate, high_gate)
    own_up = merged(train_up, low_up, high_up)
    own = (jnp.stack([own_down, own_gate]), own_up[None])
    own = lax.optimization_barrier(own)
    held = [{(0, 0): piece} for piece in own]
    for senders in ROUNDS:
        for k in range(len(own)):
            for direction, place in enumerate(senders):
                got = lax.ppermute(held[k][place], "fsdp", HOPS[direction])
                held[k][reached(direction, place)] = got
    zero = jnp.uint32(0)
    stacks = [empty() for _ in range(3)]
    for place in held[0]:
        parts = (held[0][place][:1], held[0][place][1:], held[1][place])
        for i, part in enumerate(parts):
            stacks[i] = lax.dynamic_update_slice(
                stacks[i], part, (slot(place), zero, zero)
            )
    down, gate, up = (stack.reshape(3584, COLS) for stack in stacks)
    return gate, up, down.T, serve_norm


def empty():
    return pl.pallas_call(
        lambda out_ref: None,
        out_specs=pl.BlockSpec(memory_space=pltpu.HBM),
        out_shape=jax.ShapeDtypeStruct((16, ROWS, COLS), jnp.bfloat16),
        compiler_params=pltpu.CompilerParams(has_side_effects=True),
        name="empty",
    )()


def solution(mesh):
    return jax.shard_map(
        per_device,
        mesh=mesh,
        in_specs=(
            P("fsdp", "cols"),
            P("fsdp", None),
            P(None, "cols"),
            P("fsdp", "cols"),
            P("fsdp", None),
            P(None, "cols"),
            P("cols", "fsdp"),
            P("cols", None),
            P(None, "fsdp"),
            P(("fsdp", "cols")),
            P(("fsdp", "cols")),
        ),
        out_specs=(P(None, "cols"), P(None, "cols"), P("cols", None), P()),
        check_vma=False,
    )
```

```python
import jax
import jax.numpy as jnp
from jax import lax
from jax.experimental import pallas as pl
from jax.experimental.pallas import tpu as pltpu
from jax.sharding import PartitionSpec as P


mix_rate = 1.0
Z, H = 8, 2
ROWS, COLS = 224, 896

ROUNDS = (
    ((0, 0), (0, 0), (0, 0)),
    ((1, 0), (-1, 0), (1, 0)),
    ((2, 0), (-2, 0), (-2, 0)),
    ((3, 0), (-2, 1), (2, 0)),
    ((2, 1), (-3, 1), (-1, 0)),
)
UP = [(z * H + h, (z + 1) % Z * H + h) for z in range(Z) for h in range(H)]
DOWN = [(z * H + h, (z - 1) % Z * H + h) for z in range(Z) for h in range(H)]
ACROSS = [(z * H + h, z * H + 1 - h) for z in range(Z) for h in range(H)]
HOPS = (UP, DOWN, ACROSS)


def reached(direction, place):
    dz, h = place
    return ((dz + 1, h), (dz - 1, h), (dz, 1 - h))[direction]


def merged(base, low, high):
    return (
        base.astype(jnp.float32)
        + mix_rate * jnp.dot(low, high, preferred_element_type=jnp.float32)
    ).astype(jnp.bfloat16)


def exchange(stage, total):
    name, bit = stage
    got = lax.ppermute(total, name, [(i, i ^ bit) for i in range(16)])
    return total + got


STAGES = (
    ("cols", 8),
    ("cols", 1),
    ("cols", 2),
    ("cols", 4),
    ("fsdp", 1),
    ("fsdp", 2),
    ("fsdp", 4),
    ("fsdp", 8),
)


def gather_norm(norm_train, norm_step):
    own = (norm_train + norm_step).astype(jnp.bfloat16)
    at = lax.axis_index("fsdp") * 16 + lax.axis_index("cols")
    total = lax.dynamic_update_slice(
        jnp.zeros((3584,), own.dtype), own, (at.astype(jnp.uint32) * 14,)
    )
    for stage in STAGES:
        total = exchange(stage, total)
    return total


def per_device(
    train_gate,
    low_gate,
    high_gate,
    train_up,
    low_up,
    high_up,
    train_down,
    low_down,
    high_down,
    norm_train,
    norm_step,
):
    me = lax.axis_index("fsdp").astype(jnp.uint32)

    def slot(place):
        return (((me >> 1) + (Z - place[0])) & 7) * 2 + ((me & 1) ^ place[1])

    serve_norm = gather_norm(norm_train, norm_step)
    own_down = merged(train_down.T, high_down.T, low_down.T)[None]
    own_rest = jnp.stack(
        [
            merged(train_gate, low_gate, high_gate),
            merged(train_up, low_up, high_up),
        ]
    )
    own = tuple(map(lax.optimization_barrier, (own_down, own_rest)))
    zero = jnp.uint32(0)
    down, gate, up = (empty() for _ in range(3))

    def put(stack, piece, place):
        return lax.dynamic_update_slice(stack, piece, (slot(place), zero, zero))

    down = put(down, own[0], (0, 0))
    gate = put(gate, own[1][:1], (0, 0))
    up = put(up, own[1][1:], (0, 0))
    held = [{(0, 0): piece} for piece in own]
    for number, senders in enumerate(ROUNDS):
        for k in range(2):
            for direction, place in enumerate(senders):
                got = lax.ppermute(held[k][place], "fsdp", HOPS[direction])
                there = reached(direction, place)
                held[k][there] = got
                if k == 0:
                    down = put(down, got, there)
                else:
                    gate = put(gate, got[:1], there)
                    up = put(up, got[1:], there)
            if (number, k) == (4, 0):
                down = down.reshape(3584, COLS).T
                gate, up, down = lax.optimization_barrier((gate, up, down))
    return gate.reshape(3584, COLS), up.reshape(3584, COLS), down, serve_norm


def empty():
    return pl.pallas_call(
        lambda out_ref: None,
        out_specs=pl.BlockSpec(memory_space=pltpu.HBM),
        out_shape=jax.ShapeDtypeStruct((16, ROWS, COLS), jnp.bfloat16),
        compiler_params=pltpu.CompilerParams(has_side_effects=True),
        name="empty",
    )()


def solution(mesh):
    return jax.shard_map(
        per_device,
        mesh=mesh,
        in_specs=(
            P("fsdp", "cols"),
            P("fsdp", None),
            P(None, "cols"),
            P("fsdp", "cols"),
            P("fsdp", None),
            P(None, "cols"),
            P("cols", "fsdp"),
            P("cols", None),
            P(None, "fsdp"),
            P(("fsdp", "cols")),
            P(("fsdp", "cols")),
        ),
        out_specs=(P(None, "cols"), P(None, "cols"), P("cols", None), P()),
        check_vma=False,
    )
```

```python
import jax
import jax.numpy as jnp
from jax import lax
from jax.experimental import pallas as pl
from jax.experimental.pallas import tpu as pltpu
from jax.sharding import PartitionSpec as P


mix_rate = 1.0
Z, H = 8, 2
ROWS, COLS = 224, 896

ROUNDS = (
    ((0, 0), (0, 0), (0, 0)),
    ((1, 0), (-1, 0), (1, 0)),
    ((2, 0), (-2, 0), (-2, 0)),
    ((3, 0), (-2, 1), (2, 0)),
    ((2, 1), (-3, 1), (-1, 0)),
)
UP = [(z * H + h, (z + 1) % Z * H + h) for z in range(Z) for h in range(H)]
DOWN = [(z * H + h, (z - 1) % Z * H + h) for z in range(Z) for h in range(H)]
ACROSS = [(z * H + h, z * H + 1 - h) for z in range(Z) for h in range(H)]
HOPS = (UP, DOWN, ACROSS)


def reached(direction, place):
    dz, h = place
    return ((dz + 1, h), (dz - 1, h), (dz, 1 - h))[direction]


def merged(base, low, high):
    return (
        base.astype(jnp.float32)
        + mix_rate * jnp.dot(low, high, preferred_element_type=jnp.float32)
    ).astype(jnp.bfloat16)


STAGES = (
    ("cols", (1,)),
    ("cols", (2,)),
    ("cols", (4,)),
    ("y", (1, 2, 3)),
    ("fsdp", (2, 4, 6)),
    ("fsdp", (8,)),
)


def flipped(name, bits):
    if name != "y":
        return name, [(i, i ^ bits) for i in range(16)]
    high, low = bits >> 1, bits & 1
    return ("fsdp", "cols"), [(i, i ^ (high * 16 + low * 8)) for i in range(256)]


def gather_norm(norm_train, norm_step):
    own = (norm_train + norm_step).astype(jnp.bfloat16)
    at = lax.axis_index("fsdp") * 16 + lax.axis_index("cols")
    total = lax.dynamic_update_slice(
        jnp.zeros((3584,), own.dtype), own, (at.astype(jnp.uint32) * 14,)
    )
    for name, flips in STAGES:
        got = [total]
        for bits in flips:
            got.append(lax.ppermute(total, *flipped(name, bits)))
        total = sum(got[1:], got[0])
    return total


def per_device(
    train_gate,
    low_gate,
    high_gate,
    train_up,
    low_up,
    high_up,
    train_down,
    low_down,
    high_down,
    norm_train,
    norm_step,
):
    me = lax.axis_index("fsdp").astype(jnp.uint32)

    def slot(place):
        return (((me >> 1) + (Z - place[0])) & 7) * 2 + ((me & 1) ^ place[1])

    serve_norm = gather_norm(norm_train, norm_step)
    own_down = merged(train_down.T, high_down.T, low_down.T)[None]
    own_rest = jnp.stack(
        [
            merged(train_gate, low_gate, high_gate),
            merged(train_up, low_up, high_up),
        ]
    )
    own = tuple(map(lax.optimization_barrier, (own_down, own_rest)))
    zero = jnp.uint32(0)
    down, gate, up = empty(3)

    def put(stack, piece, place):
        return lax.dynamic_update_slice(stack, piece, (slot(place), zero, zero))

    down = put(down, own[0], (0, 0))
    gate = put(gate, own[1][:1], (0, 0))
    up = put(up, own[1][1:], (0, 0))
    held = [{(0, 0): piece} for piece in own]
    for number, senders in enumerate(ROUNDS):
        for k in range(2):
            for direction, place in enumerate(senders):
                got = lax.ppermute(held[k][place], "fsdp", HOPS[direction])
                there = reached(direction, place)
                held[k][there] = got
                if k == 0:
                    down = put(down, got, there)
                else:
                    gate = put(gate, got[:1], there)
                    up = put(up, got[1:], there)
            if (number, k) == (4, 0):
                down = turned(
                    pltpu.with_memory_space_constraint(
                        down.reshape(3584, COLS), pltpu.HBM
                    )
                )
                gate, up, down = lax.optimization_barrier((gate, up, down))
    return gate.reshape(3584, COLS), up.reshape(3584, COLS), down, serve_norm


def empty(count):
    return pl.pallas_call(
        lambda *out_refs: None,
        out_specs=[pl.BlockSpec(memory_space=pltpu.HBM)] * count,
        out_shape=[pltpu.HBM((16, ROWS, COLS), jnp.bfloat16)] * count,
        compiler_params=pltpu.CompilerParams(
            has_side_effects=True, vmem_limit_bytes=1 << 20
        ),
        name="empty",
    )()


def turn_kernel(in_ref, out_ref):
    out_ref[...] = in_ref[...].T


def turned(x):
    rows, cols = x.shape
    return pl.pallas_call(
        turn_kernel,
        grid=(rows // 512,),
        in_specs=[pl.BlockSpec((512, cols), lambda i: (i, 0))],
        out_specs=pl.BlockSpec((cols, 512), lambda i: (0, i)),
        out_shape=jax.ShapeDtypeStruct((cols, rows), x.dtype),
        compiler_params=pltpu.CompilerParams(vmem_limit_bytes=16 << 20),
        cost_estimate=pl.CostEstimate(
            flops=1 << 33, bytes_accessed=4 * rows * cols, transcendentals=0
        ),
        name="turn",
    )(x)


def solution(mesh):
    return jax.shard_map(
        per_device,
        mesh=mesh,
        in_specs=(
            P("fsdp", "cols"),
            P("fsdp", None),
            P(None, "cols"),
            P("fsdp", "cols"),
            P("fsdp", None),
            P(None, "cols"),
            P("cols", "fsdp"),
            P("cols", None),
            P(None, "fsdp"),
            P(("fsdp", "cols")),
            P(("fsdp", "cols")),
        ),
        out_specs=(P(None, "cols"), P(None, "cols"), P("cols", None), P()),
        check_vma=False,
    )
```

```python
import jax
import jax.numpy as jnp
from jax import lax
from jax.experimental import pallas as pl
from jax.experimental.pallas import tpu as pltpu
from jax.sharding import PartitionSpec as P


mix_rate = 1.0
Z, H = 8, 2
ROWS, COLS = 224, 896

ROUNDS = (
    ((0, 0), (0, 0), (0, 0)),
    ((1, 0), (1, 0), (-1, 0)),
    ((-2, 0), (2, 0), (-2, 0)),
    ((2, 0), (3, 0), (-2, 1)),
    ((-1, 0), (2, 1), (-3, 1)),
)


def along(step):
    pairs = []
    for i in range(256):
        z, h, c = i // 32, i // 16 % H, i % 16
        pairs.append((i, ((z + (-step if c % 2 else step)) % Z * H + h) * 16 + c))
    return ("fsdp", "cols"), pairs


ACROSS = "fsdp", [(i, i ^ 1) for i in range(16)]
HOPS = (ACROSS, along(1), along(-1))
TURNS = ((1, 0, 2), (2, 0, 1))


def reached(direction, place):
    dz, h = place
    return ((dz, 1 - h), (dz + 1, h), (dz - 1, h))[direction]


def merged(base, low, high):
    return (
        base.astype(jnp.float32)
        + mix_rate * jnp.dot(low, high, preferred_element_type=jnp.float32)
    ).astype(jnp.bfloat16)


STAGES = (
    ("cols", (1,)),
    ("cols", (2,)),
    ("cols", (4,)),
    ("y", (1, 2, 3)),
    ("fsdp", (2, 4, 6)),
    ("fsdp", (8,)),
)


def merge_kernel(base_hbm, lhs_hbm, rhs_hbm, out_ref, base, lhs, rhs, sems):
    loads = [
        pltpu.make_async_copy(lhs_hbm, lhs, sems.at[0]),
        pltpu.make_async_copy(rhs_hbm, rhs, sems.at[1]),
    ]
    parts = (slice(0, 384), slice(384, COLS))
    for i, part in enumerate(parts):
        loads.append(
            pltpu.make_async_copy(
                base_hbm.at[:, part], base.at[:, part], sems.at[2 + i]
            )
        )
    for load in loads:
        load.start()
    loads[0].wait()
    loads[1].wait()
    for i, part in enumerate(parts):
        added = lax.dot_general(
            lhs[...],
            rhs[:, part],
            (((0,), (0,)), ((), ())),
            preferred_element_type=jnp.float32,
        )
        loads[2 + i].wait()
        out_ref[0, :, part] = (
            base[:, part].astype(jnp.float32) + mix_rate * added
        ).astype(jnp.bfloat16)


def merged_by_kernel(base, lhs, rhs):
    operands = (base, lhs, rhs)
    return pl.pallas_call(
        merge_kernel,
        in_specs=[pl.BlockSpec(memory_space=pltpu.HBM)] * 3,
        out_specs=pl.BlockSpec(memory_space=pltpu.VMEM),
        out_shape=pltpu.VMEM((1, ROWS, COLS), jnp.bfloat16),
        scratch_shapes=[pltpu.VMEM(x.shape, x.dtype) for x in operands]
        + [pltpu.SemaphoreType.DMA((4,))],
        compiler_params=pltpu.CompilerParams(vmem_limit_bytes=8 << 20),
        cost_estimate=pl.CostEstimate(
            flops=2 * ROWS * COLS * 16, bytes_accessed=1 << 20, transcendentals=0
        ),
        name="merge",
    )(*(pltpu.with_memory_space_constraint(x, pltpu.HBM) for x in operands))


def flipped(name, bits):
    if name != "y":
        return name, [(i, i ^ bits) for i in range(16)]
    high, low = bits >> 1, bits & 1
    return ("fsdp", "cols"), [(i, i ^ (high * 16 + low * 8)) for i in range(256)]


def gather_norm(norm_train, norm_step):
    own = (norm_train + norm_step).astype(jnp.bfloat16)
    at = lax.axis_index("fsdp") * 16 + lax.axis_index("cols")
    total = lax.dynamic_update_slice(
        jnp.zeros((3584,), own.dtype), own, (at.astype(jnp.uint32) * 14,)
    )
    for name, flips in STAGES:
        got = [total]
        for bits in flips:
            got.append(lax.ppermute(total, *flipped(name, bits)))
        total = sum(got[1:], got[0])
    return total


def per_device(
    train_gate,
    low_gate,
    high_gate,
    train_up,
    low_up,
    high_up,
    train_down,
    low_down,
    high_down,
    norm_train,
    norm_step,
):
    me = lax.axis_index("fsdp").astype(jnp.uint32)
    core = lax.axis_index("cols").astype(jnp.uint32) & 1
    back = 1 - 2 * core

    def slot(place):
        z = ((me >> 1) + back * (Z - place[0])) & (Z - 1)
        return z * H + ((me & 1) ^ place[1])

    serve_norm = gather_norm(norm_train, norm_step)
    own_down = merged_by_kernel(train_down.T, high_down, low_down.T)
    own_rest = jnp.stack(
        [
            merged(train_gate, low_gate, high_gate),
            merged(train_up, low_up, high_up),
        ]
    )
    own = tuple(map(lax.optimization_barrier, (own_down, own_rest)))
    zero = jnp.uint32(0)
    down, gate, up = empty(3)

    def put(stack, piece, place):
        return lax.dynamic_update_slice(stack, piece, (slot(place), zero, zero))

    down = put(down, own[0], (0, 0))
    gate = put(gate, own[1][:1], (0, 0))
    up = put(up, own[1][1:], (0, 0))
    held = [{(0, 0): piece} for piece in own]
    for number, senders in enumerate(ROUNDS):
        for k in range(2):
            for direction, place in enumerate(senders):
                got = lax.ppermute(held[k][place], *HOPS[direction])
                held[k][reached(direction, place)] = got
            if (number, k) == (4, 1):
                there = [reached(d, place) for d, place in enumerate(senders)]
                gate, up = put_last(
                    gate, up, [held[1][t] for t in there], [slot(t) for t in there]
                )
                break
            for direction in TURNS[0]:
                there = reached(direction, senders[direction])
                got = held[k][there]
                if k == 0:
                    down = put(down, got, there)
                else:
                    gate = put(gate, got[:1], there)
                    up = put(up, got[1:], there)
            if (number, k) == (4, 0):
                down = turned(
                    pltpu.with_memory_space_constraint(
                        down.reshape(3584, COLS), pltpu.HBM
                    )
                )
                gate, up, down = lax.optimization_barrier((gate, up, down))
    return gate.reshape(3584, COLS), up.reshape(3584, COLS), down, serve_norm


def put_last_kernel(slots, *refs):
    pieces, stacks, sems = refs[2:5], refs[5:7], refs[7]
    copies = [
        pltpu.make_async_copy(piece.at[i], stack.at[slots[d]], sems.at[d, i])
        for d, piece in enumerate(pieces)
        for i, stack in enumerate(stacks)
    ]
    for copy in copies:
        copy.start()
    for copy in copies:
        copy.wait()


def put_last(gate, up, pieces, slots):
    anywhere = pl.BlockSpec(memory_space=pl.ANY)
    return pl.pallas_call(
        put_last_kernel,
        in_specs=[pl.BlockSpec(memory_space=pltpu.SMEM)] + [anywhere] * 5,
        out_specs=[anywhere] * 2,
        out_shape=[jax.ShapeDtypeStruct(x.shape, x.dtype) for x in (gate, up)],
        input_output_aliases={1: 0, 2: 1},
        scratch_shapes=[pltpu.SemaphoreType.DMA((3, 2))],
        compiler_params=pltpu.CompilerParams(vmem_limit_bytes=1 << 20),
        cost_estimate=pl.CostEstimate(
            flops=1 << 20, bytes_accessed=12 * ROWS * COLS * 2, transcendentals=0
        ),
        name="put_last",
    )(jnp.stack(slots).astype(jnp.int32), gate, up, *pieces)


def empty(count):
    return pl.pallas_call(
        lambda *out_refs: None,
        out_specs=[pl.BlockSpec(memory_space=pltpu.HBM)] * count,
        out_shape=[pltpu.HBM((16, ROWS, COLS), jnp.bfloat16)] * count,
        compiler_params=pltpu.CompilerParams(
            has_side_effects=True, vmem_limit_bytes=1 << 20
        ),
        name="empty",
    )()


def turn_kernel(in_ref, out_ref):
    out_ref[...] = in_ref[...].T


def turned(x):
    rows, cols = x.shape
    return pl.pallas_call(
        turn_kernel,
        grid=(rows // 512,),
        in_specs=[pl.BlockSpec((512, cols), lambda i: (i, 0))],
        out_specs=pl.BlockSpec((cols, 512), lambda i: (0, i)),
        out_shape=jax.ShapeDtypeStruct((cols, rows), x.dtype),
        compiler_params=pltpu.CompilerParams(vmem_limit_bytes=16 << 20),
        cost_estimate=pl.CostEstimate(
            flops=1 << 33, bytes_accessed=4 * rows * cols, transcendentals=0
        ),
        name="turn",
    )(x)


def solution(mesh):
    return jax.shard_map(
        per_device,
        mesh=mesh,
        in_specs=(
            P("fsdp", "cols"),
            P("fsdp", None),
            P(None, "cols"),
            P("fsdp", "cols"),
            P("fsdp", None),
            P(None, "cols"),
            P("cols", "fsdp"),
            P("cols", None),
            P(None, "fsdp"),
            P(("fsdp", "cols")),
            P(("fsdp", "cols")),
        ),
        out_specs=(P(None, "cols"), P(None, "cols"), P("cols", None), P()),
        check_vma=False,
    )
```

```python
import jax
import jax.numpy as jnp
from jax import lax
from jax.experimental import pallas as pl
from jax.experimental.pallas import tpu as pltpu
from jax.sharding import PartitionSpec as P


mix_rate = 1.0
Z, H = 8, 2
ROWS, COLS = 224, 896

ROUNDS = (
    ((0, 0), (0, 0), (0, 0)),
    ((1, 0), (1, 0), (-1, 0)),
    ((-2, 0), (2, 0), (-2, 0)),
    ((2, 0), (3, 0), (-2, 1)),
    ((-1, 0), (2, 1), (-3, 1)),
)


def along(step):
    pairs = []
    for i in range(256):
        z, h, c = i // 32, i // 16 % H, i % 16
        pairs.append((i, ((z + (-step if c % 2 else step)) % Z * H + h) * 16 + c))
    return ("fsdp", "cols"), pairs


ACROSS = "fsdp", [(i, i ^ 1) for i in range(16)]
HOPS = (ACROSS, along(1), along(-1))


def reached(direction, place):
    dz, h = place
    return ((dz, 1 - h), (dz + 1, h), (dz - 1, h))[direction]


def merged(base, low, high):
    return (
        base.astype(jnp.float32)
        + mix_rate * jnp.dot(low, high, preferred_element_type=jnp.float32)
    ).astype(jnp.bfloat16)


STAGES = (
    ("cols", (1,)),
    ("cols", (2,)),
    ("cols", (4,)),
    ("y", (1, 2, 3)),
    ("fsdp", (2, 4, 6)),
    ("fsdp", (8,)),
)


def merge_kernel(base_hbm, lhs_hbm, rhs_hbm, out_ref, base, lhs, rhs, added, sems):
    loads = [
        pltpu.make_async_copy(lhs_hbm, lhs, sems.at[0]),
        pltpu.make_async_copy(rhs_hbm, rhs, sems.at[1]),
    ]
    parts = [slice(at, min(at + 256, COLS)) for at in range(0, COLS, 256)]
    for i, part in enumerate(parts):
        loads.append(
            pltpu.make_async_copy(
                base_hbm.at[:, part], base.at[:, part], sems.at[2 + i]
            )
        )
    for load in loads:
        load.start()
    loads[0].wait()
    loads[1].wait()
    added[...] = lax.dot_general(
        lhs[...], rhs[...], (((0,), (0,)), ((), ())), preferred_element_type=jnp.float32
    )
    for i, part in enumerate(parts):
        loads[2 + i].wait()
        out_ref[0, :, part] = (
            base[:, part].astype(jnp.float32) + mix_rate * added[:, part]
        ).astype(jnp.bfloat16)


def merged_by_kernel(base, lhs, rhs):
    operands = (base, lhs, rhs)
    return pl.pallas_call(
        merge_kernel,
        in_specs=[pl.BlockSpec(memory_space=pltpu.HBM)] * 3,
        out_specs=pl.BlockSpec(memory_space=pltpu.VMEM),
        out_shape=pltpu.VMEM((1, ROWS, COLS), jnp.bfloat16),
        scratch_shapes=[pltpu.VMEM(x.shape, x.dtype) for x in operands]
        + [pltpu.VMEM((ROWS, COLS), jnp.float32), pltpu.SemaphoreType.DMA((6,))],
        compiler_params=pltpu.CompilerParams(vmem_limit_bytes=8 << 20),
        cost_estimate=pl.CostEstimate(
            flops=2 * ROWS * COLS * 16, bytes_accessed=1 << 20, transcendentals=0
        ),
        name="merge",
    )(*(pltpu.with_memory_space_constraint(x, pltpu.HBM) for x in operands))


def flipped(name, bits):
    if name != "y":
        return name, [(i, i ^ bits) for i in range(16)]
    high, low = bits >> 1, bits & 1
    return ("fsdp", "cols"), [(i, i ^ (high * 16 + low * 8)) for i in range(256)]


def gather_norm(norm_train, norm_step):
    own = (norm_train + norm_step).astype(jnp.bfloat16)
    at = lax.axis_index("fsdp") * 16 + lax.axis_index("cols")
    total = lax.dynamic_update_slice(
        jnp.zeros((3584,), own.dtype), own, (at.astype(jnp.uint32) * 14,)
    )
    for name, flips in STAGES:
        got = [total]
        for bits in flips:
            got.append(lax.ppermute(total, *flipped(name, bits)))
        total = sum(got[1:], got[0])
    return total


def per_device(
    train_gate,
    low_gate,
    high_gate,
    train_up,
    low_up,
    high_up,
    train_down,
    low_down,
    high_down,
    norm_train,
    norm_step,
):
    me = lax.axis_index("fsdp").astype(jnp.uint32)
    core = lax.axis_index("cols").astype(jnp.uint32) & 1
    back = 1 - 2 * core

    def slot(place):
        z = ((me >> 1) + back * (Z - place[0])) & (Z - 1)
        return z * H + ((me & 1) ^ place[1])

    serve_norm = gather_norm(norm_train, norm_step)
    own_down = merged_by_kernel(train_down.T, high_down, low_down.T)
    own_rest = jnp.stack(
        [
            merged(train_gate, low_gate, high_gate),
            merged(train_up, low_up, high_up),
        ]
    )
    own = tuple(map(lax.optimization_barrier, (own_down, own_rest)))
    zero = jnp.uint32(0)
    down, gate, up = empty(3)

    def put(stack, piece, place):
        return lax.dynamic_update_slice(stack, piece, (slot(place), zero, zero))

    down = put(down, own[0], (0, 0))
    gate = put(gate, own[1][:1], (0, 0))
    up = put(up, own[1][1:], (0, 0))
    held = [{(0, 0): piece} for piece in own]
    for number, senders in enumerate(ROUNDS):
        for k in range(2):
            for direction, place in enumerate(senders):
                got = lax.ppermute(held[k][place], *HOPS[direction])
                held[k][reached(direction, place)] = got
            for direction in (2, 0, 1):
                there = reached(direction, senders[direction])
                got = held[k][there]
                if k == 0:
                    down = put(down, got, there)
                else:
                    gate = put(gate, got[:1], there)
                    up = put(up, got[1:], there)
            if (number, k) == (4, 0):
                down = turned(
                    pltpu.with_memory_space_constraint(
                        down.reshape(3584, COLS), pltpu.HBM
                    )
                )
                gate, up, down = lax.optimization_barrier((gate, up, down))
    return gate.reshape(3584, COLS), up.reshape(3584, COLS), down, serve_norm


def empty(count):
    return pl.pallas_call(
        lambda *out_refs: None,
        out_specs=[pl.BlockSpec(memory_space=pltpu.HBM)] * count,
        out_shape=[pltpu.HBM((16, ROWS, COLS), jnp.bfloat16)] * count,
        compiler_params=pltpu.CompilerParams(
            has_side_effects=True, vmem_limit_bytes=1 << 20
        ),
        name="empty",
    )()


def turn_kernel(in_ref, out_ref):
    out_ref[...] = in_ref[...].T


def turned(x):
    rows, cols = x.shape
    return pl.pallas_call(
        turn_kernel,
        grid=(rows // 512,),
        in_specs=[pl.BlockSpec((512, cols), lambda i: (i, 0))],
        out_specs=pl.BlockSpec((cols, 512), lambda i: (0, i)),
        out_shape=jax.ShapeDtypeStruct((cols, rows), x.dtype),
        compiler_params=pltpu.CompilerParams(vmem_limit_bytes=16 << 20),
        cost_estimate=pl.CostEstimate(
            flops=1 << 33, bytes_accessed=4 * rows * cols, transcendentals=0
        ),
        name="turn",
    )(x)


def solution(mesh):
    return jax.shard_map(
        per_device,
        mesh=mesh,
        in_specs=(
            P("fsdp", "cols"),
            P("fsdp", None),
            P(None, "cols"),
            P("fsdp", "cols"),
            P("fsdp", None),
            P(None, "cols"),
            P("cols", "fsdp"),
            P("cols", None),
            P(None, "fsdp"),
            P(("fsdp", "cols")),
            P(("fsdp", "cols")),
        ),
        out_specs=(P(None, "cols"), P(None, "cols"), P("cols", None), P()),
        check_vma=False,
    )
```

```python
import functools

import jax
import jax.numpy as jnp
from jax import lax
from jax.experimental import pallas as pl
from jax.experimental.pallas import tpu as pltpu
from jax.sharding import PartitionSpec as P


mix_rate = 1.0
Z, H = 8, 2
ROWS, COLS = 224, 896

ROUNDS = (
    ((0, 0), (0, 0), (0, 0)),
    ((1, 0), (1, 0), (-1, 0)),
    ((-2, 0), (2, 0), (-2, 0)),
    ((2, 0), (3, 0), (-2, 1)),
    ((-1, 0), (2, 1), (-3, 1)),
)


def along(step):
    pairs = []
    for i in range(256):
        z, h, c = i // 32, i // 16 % H, i % 16
        pairs.append((i, ((z + (-step if c % 2 else step)) % Z * H + h) * 16 + c))
    return ("fsdp", "cols"), pairs


ACROSS = "fsdp", [(i, i ^ 1) for i in range(16)]
HOPS = (ACROSS, along(1), along(-1))


def reached(direction, place):
    dz, h = place
    return ((dz, 1 - h), (dz + 1, h), (dz - 1, h))[direction]


STAGES = (
    ("cols", (1,)),
    ("cols", (2,)),
    ("cols", (4,)),
    ("y", (1, 2, 3)),
    ("fsdp", (2, 4, 6)),
    ("fsdp", (8,)),
)


PARTS = [slice(at, min(at + 256, COLS)) for at in range(0, COLS, 256)]


def merge_kernel(count, *refs):
    sources, out_ref = refs[: 3 * count], refs[3 * count]
    held, (added, sems) = refs[3 * count + 1 : 6 * count + 1], refs[6 * count + 1 :]
    loads = []
    for n in range(count):
        base_hbm, lhs_hbm, rhs_hbm = sources[3 * n : 3 * n + 3]
        base, lhs, rhs = held[3 * n : 3 * n + 3]
        loads.append(
            [
                pltpu.make_async_copy(lhs_hbm, lhs, sems.at[n, 0]),
                pltpu.make_async_copy(rhs_hbm, rhs, sems.at[n, 1]),
            ]
            + [
                pltpu.make_async_copy(
                    base_hbm.at[:, part], base.at[:, part], sems.at[n, 2 + i]
                )
                for i, part in enumerate(PARTS)
            ]
        )
        for load in loads[n]:
            load.start()
    for n in range(count):
        base, lhs, rhs = held[3 * n : 3 * n + 3]
        loads[n][0].wait()
        loads[n][1].wait()
        added[...] = lax.dot_general(
            lhs[...],
            rhs[...],
            (((0,), (0,)), ((), ())),
            preferred_element_type=jnp.float32,
        )
        for i, part in enumerate(PARTS):
            loads[n][2 + i].wait()
            out_ref[n, :, part] = (
                base[:, part].astype(jnp.float32) + mix_rate * added[:, part]
            ).astype(jnp.bfloat16)


def merged_by_kernel(*operands):
    count = len(operands) // 3
    return pl.pallas_call(
        functools.partial(merge_kernel, count),
        in_specs=[pl.BlockSpec(memory_space=pltpu.HBM)] * len(operands),
        out_specs=pl.BlockSpec(memory_space=pltpu.VMEM),
        out_shape=pltpu.VMEM((count, ROWS, COLS), jnp.bfloat16),
        scratch_shapes=[pltpu.VMEM(x.shape, x.dtype) for x in operands]
        + [
            pltpu.VMEM((ROWS, COLS), jnp.float32),
            pltpu.SemaphoreType.DMA((count, 2 + len(PARTS))),
        ],
        compiler_params=pltpu.CompilerParams(vmem_limit_bytes=8 << 20),
        cost_estimate=pl.CostEstimate(
            flops=2 * count * ROWS * COLS * 16,
            bytes_accessed=count << 20,
            transcendentals=0,
        ),
    )(*(pltpu.with_memory_space_constraint(x, pltpu.HBM) for x in operands))


def flipped(name, bits):
    if name != "y":
        return name, [(i, i ^ bits) for i in range(16)]
    high, low = bits >> 1, bits & 1
    return ("fsdp", "cols"), [(i, i ^ (high * 16 + low * 8)) for i in range(256)]


def gather_norm(norm_train, norm_step):
    own = (norm_train + norm_step).astype(jnp.bfloat16)
    at = lax.axis_index("fsdp") * 16 + lax.axis_index("cols")
    total = lax.dynamic_update_slice(
        jnp.zeros((3584,), own.dtype), own, (at.astype(jnp.uint32) * 14,)
    )
    for name, flips in STAGES:
        got = [total]
        for bits in flips:
            got.append(lax.ppermute(total, *flipped(name, bits)))
        total = sum(got[1:], got[0])
    return total


def per_device(
    train_gate,
    low_gate,
    high_gate,
    train_up,
    low_up,
    high_up,
    train_down,
    low_down,
    high_down,
    norm_train,
    norm_step,
):
    me = lax.axis_index("fsdp").astype(jnp.uint32)
    core = lax.axis_index("cols").astype(jnp.uint32) & 1
    back = 1 - 2 * core

    def slot(place):
        z = ((me >> 1) + back * (Z - place[0])) & (Z - 1)
        return z * H + ((me & 1) ^ place[1])

    serve_norm = gather_norm(norm_train, norm_step)
    own_down = merged_by_kernel(train_down.T, high_down, low_down.T)
    own_rest = merged_by_kernel(
        train_gate, low_gate.T, high_gate, train_up, low_up.T, high_up
    )
    own = tuple(map(lax.optimization_barrier, (own_down, own_rest)))
    zero = jnp.uint32(0)
    down, gate, up = empty(3)

    def put(stack, piece, place):
        return lax.dynamic_update_slice(stack, piece, (slot(place), zero, zero))

    down = put(down, own[0], (0, 0))
    gate = put(gate, own[1][:1], (0, 0))
    up = put(up, own[1][1:], (0, 0))
    held = [{(0, 0): piece} for piece in own]
    for number, senders in enumerate(ROUNDS):
        for k in range(2):
            for direction, place in enumerate(senders):
                got = lax.ppermute(held[k][place], *HOPS[direction])
                held[k][reached(direction, place)] = got
            for direction in (2, 0, 1):
                there = reached(direction, senders[direction])
                got = held[k][there]
                if k == 0:
                    down = put(down, got, there)
                else:
                    gate = put(gate, got[:1], there)
                    up = put(up, got[1:], there)
            if (number, k) == (4, 0):
                down = turned(
                    pltpu.with_memory_space_constraint(
                        down.reshape(3584, COLS), pltpu.HBM
                    )
                )
                gate, up, down = lax.optimization_barrier((gate, up, down))
    return gate.reshape(3584, COLS), up.reshape(3584, COLS), down, serve_norm


def empty(count):
    return pl.pallas_call(
        lambda *out_refs: None,
        out_specs=[pl.BlockSpec(memory_space=pltpu.HBM)] * count,
        out_shape=[pltpu.HBM((16, ROWS, COLS), jnp.bfloat16)] * count,
        compiler_params=pltpu.CompilerParams(
            has_side_effects=True, vmem_limit_bytes=1 << 20
        ),
        name="empty",
    )()


def turn_kernel(in_ref, out_ref):
    out_ref[...] = in_ref[...].T


def turned(x):
    rows, cols = x.shape
    return pl.pallas_call(
        turn_kernel,
        grid=(rows // 512,),
        in_specs=[pl.BlockSpec((512, cols), lambda i: (i, 0))],
        out_specs=pl.BlockSpec((cols, 512), lambda i: (0, i)),
        out_shape=jax.ShapeDtypeStruct((cols, rows), x.dtype),
        compiler_params=pltpu.CompilerParams(vmem_limit_bytes=16 << 20),
        cost_estimate=pl.CostEstimate(
            flops=1 << 33, bytes_accessed=4 * rows * cols, transcendentals=0
        ),
        name="turn",
    )(x)


def solution(mesh):
    return jax.shard_map(
        per_device,
        mesh=mesh,
        in_specs=(
            P("fsdp", "cols"),
            P("fsdp", None),
            P(None, "cols"),
            P("fsdp", "cols"),
            P("fsdp", None),
            P(None, "cols"),
            P("cols", "fsdp"),
            P("cols", None),
            P(None, "fsdp"),
            P(("fsdp", "cols")),
            P(("fsdp", "cols")),
        ),
        out_specs=(P(None, "cols"), P(None, "cols"), P("cols", None), P()),
        check_vma=False,
    )
```
